32 devices in a mesh: rep: 1 (over z), dp: 32 (over x, y, core).
Axes of the slice: x: 4, y: 4, z: 1, core: 2. Of those that a mesh axis runs over, the one named last changes fastest.
The devices are a block of a 4x4x8 slice.
Arguments:
- x: bfloat16 [32, 2048, 768], P(('rep', 'dp'))
- dy: bfloat16 [32, 2048, 768], P(('rep', 'dp'))
- w_gate: bfloat16 [2, 768, 2304], replicated
- w_up: bfloat16 [2, 768, 2304], replicated
- w_down: bfloat16 [2, 2304, 768], replicated
- m_w_gate: float32 [2, 768, 2304], replicated
- m_w_up: float32 [2, 768, 2304], replicated
- m_w_down: float32 [2, 2304, 768], replicated
- v_w_gate: float32 [2, 768, 2304], replicated
- v_w_up: float32 [2, 768, 2304], replicated
- v_w_down: float32 [2, 2304, 768], replicated
Outputs:
- output 1: bfloat16 [2, 768, 2304], P('rep')
- output 2: bfloat16 [2, 768, 2304], P('rep')
- output 3: bfloat16 [2, 2304, 768], P('rep')
- output 4: float32 [2, 768, 2304], P('rep')
- output 5: float32 [2, 768, 2304], P('rep')
- output 6: float32 [2, 2304, 768], P('rep')
- output 7: float32 [2, 768, 2304], P('rep')
- output 8: float32 [2, 768, 2304], P('rep')
- output 9: float32 [2, 2304, 768], P('rep')
All inputs are finite; a program needn't handle non-finite values.
Results may differ from the reference program's by a relative error of at most 0.02.
Values are sent between devices in bfloat16 or wider.
A program may use at most 768 MiB of HBM per device.

```python
import jax
import jax.numpy as jnp
from jax import lax

SEQUENCES = 32
TOKENS = 2048
D = 768
FF = 2304
LAYERS = 2
NAMES = ("w_gate", "w_up", "w_down")
SHAPES = {"w_gate": (LAYERS, D, FF), "w_up": (LAYERS, D, FF), "w_down": (LAYERS, FF, D)}


def bump(key, n, height):
    away = (jnp.arange(n, dtype=jnp.int32) - jax.random.randint(key, (), 0, n, jnp.int32)) % n
    return jnp.where(away < n // 8, height, 1.0)


def together(key, own, strength):
    shared = jax.random.normal(key, own.shape[1:], jnp.float32)
    return (own + strength * shared) * lax.rsqrt(1 + strength * strength)


def setup_inputs(seed: int = 0, part: int = 0) -> dict:
    kx, kdy, ka, kb, kz, kf, kh, kl, *keys = jax.random.split(jax.random.key(seed), 8 + 3 * len(NAMES))
    kx, kdy, ka, kb = (jax.random.fold_in(k, part) for k in (kx, kdy, ka, kb))
    kw, km, kv = (keys[i::3] for i in range(3))
    shape = (SEQUENCES, TOKENS, D)
    much_x, much_dy = jax.random.uniform(kz, (2,), jnp.float32, 0.0, 1.0)
    loud = 2.0 ** jax.random.uniform(jax.random.fold_in(kz, 1), (), jnp.float32, -1.0, 2.0)
    layers = 2.0 ** jax.random.uniform(kl, (LAYERS, 1, 1), jnp.float32, -1.0, 1.0)
    x = together(ka, jax.random.normal(kx, shape, jnp.float32), much_x) * bump(kf, D, 4.0)
    dy = together(kb, jax.random.normal(kdy, shape, jnp.float32), much_dy)
    drawn = {"x": x.astype(jnp.bfloat16), "dy": (loud * dy * (SEQUENCES * TOKENS) ** -0.5).astype(jnp.bfloat16)}
    for key, name in zip(kw, NAMES, strict=True):
        w = jax.random.normal(key, SHAPES[name], jnp.float32) * SHAPES[name][1] ** -0.5
        drawn[name] = (w * {"w_gate": 1.0, "w_up": bump(kh, FF, 4.0), "w_down": layers}[name]).astype(jnp.bfloat16)
    for key, name in zip(km, NAMES, strict=True):
        drawn[f"m_{name}"] = 0.1 * jax.random.normal(key, SHAPES[name], jnp.float32)
    for key, name in zip(kv, NAMES, strict=True):
        drawn[f"v_{name}"] = jax.random.uniform(key, SHAPES[name], jnp.float32, 0.005, 0.015)
    return drawn


def matmul(a, w):
    return jnp.dot(a, w, preferred_element_type=jnp.float32).astype(jnp.bfloat16)


def normed(h):
    wide = h.astype(jnp.float32)
    scale = lax.rsqrt(jnp.mean(wide**2, -1, keepdims=True) + 1e-6)
    return (wide * scale).astype(jnp.bfloat16)


def layer(h, w):
    a = normed(h)
    gate = jnp.dot(a, w["w_gate"], preferred_element_type=jnp.float32)
    up = jnp.dot(a, w["w_up"], preferred_element_type=jnp.float32)
    return h + matmul((jax.nn.silu(gate) * up).astype(jnp.bfloat16), w["w_down"])


def adamw(w, m, v, g):
    m = 0.9 * m + 0.1 * g
    v = 0.95 * v + 0.05 * g * g
    step = m * lax.rsqrt(v + 1e-8) + 0.1 * w
    return (w - 0.02 * step).astype(jnp.bfloat16), m, v


def stack(weights, h):
    return lax.scan(lambda h, w: (layer(h, w), None), h, weights)[0]


def reference(x, dy, w_gate, w_up, w_down, m_w_gate, m_w_up, m_w_down, v_w_gate, v_w_up, v_w_down):
    weights = dict(zip(NAMES, (w_gate, w_up, w_down), strict=True))

    def take(so_far, sequence):
        h, by_y = sequence
        _, back = jax.vjp(lambda w: stack(w, h), weights)
        return jax.tree.map(lambda total, term: total + term.astype(jnp.float32), so_far, back(by_y)[0]), None

    none_yet = {name: jnp.zeros(w.shape, jnp.float32) for name, w in weights.items()}
    by_weights, _ = lax.scan(take, none_yet, (x, dy))
    gradients = [by_weights[name].astype(jnp.bfloat16).astype(jnp.float32) for name in NAMES]
    new = [
        adamw(w.astype(jnp.float32), m, v, g)
        for w, m, v, g in zip((w_gate, w_up, w_down), (m_w_gate, m_w_up, m_w_down), (v_w_gate, v_w_up, v_w_down), gradients, strict=True)
    ]
    return tuple(one[which] for which in range(3) for one in new)
```

```python
import functools

import jax
import jax.numpy as jnp
from jax import lax
from jax.experimental import pallas as pl
from jax.experimental.pallas import tpu as pltpu
from jax.sharding import PartitionSpec as P

F32, BF16 = jnp.float32, jnp.bfloat16
STEPS = 9


class Copy:
    def __init__(self, describe):
        self.describe = describe

    def __getattr__(self, name):
        return getattr(self.describe(), name)


def summed_kernel(side, count, layout, *refs):
    lefts, rights = layout
    n_in = max(lefts) + 1 + count
    left_refs, right_refs, out = refs[: max(lefts) + 1], refs[max(lefts) + 1 : n_in], refs[n_in]
    (lv, rv, other, own, got, b1, b2, ub, cr, fb, l_sem, r_sem, a_s, a_r, b_s, b_r, c_s, c_r, d_s, d_r, e_s, e_r, f_s, f_r, o_sem) = refs[n_in + 1 :]
    rows, half = own.shape[1:]
    chunk, sub = rows // side, rows // side // side
    part = chunk // 2

    me = lax.axis_index("dp")
    core = me % 2
    x, y = me // (2 * side), me // 2 % side
    p1, p2 = x * (1 - core) + y * core, y * (1 - core) + x * core
    far, near = 2 * side * (1 - core) + 2 * core, 2 * (1 - core) + 2 * side * core

    def at(q1, q2):
        return {"dp": q1 * far + q2 * near + core}

    up, down, across = (p1 + 1) % side, (p1 + side - 1) % side, (p1 + 2) % side
    mate = {"dp": me + 1 - 2 * core}
    ups, downs = at(up, p2), at(down, p2)
    others = [at(p1, (p2 + e) % side) for e in range(1, side)]

    barrier = pltpu.get_barrier_semaphore()
    peers = [mate, ups, downs] + others
    for peer in peers:
        pl.semaphore_signal(barrier, inc=1, device_id=peer, device_id_type=pl.DeviceIdType.MESH)
    pl.semaphore_wait(barrier, len(peers))

    mine = pl.ds(pl.multiple_of(core * half, 128), half)
    theirs = pl.ds(pl.multiple_of((1 - core) * half, 128), half)

    def span(start, size):
        return pl.ds(pl.multiple_of(start, 16), size)

    def remote(src, dst, send, recv, to):
        return Copy(
            lambda: pltpu.make_async_remote_copy(
                src_ref=src, dst_ref=dst, send_sem=send, recv_sem=recv, device_id=to, device_id_type=pl.DeviceIdType.MESH
            )
        )

    def copy_a(k):
        return remote(other.at[k % 2], got.at[k], a_s.at[k], a_r.at[k], mate)

    def copies_b(k):
        return (
            remote(got.at[k, span(across * chunk, part)], b1.at[k, 0], b_s.at[k, 0], b_r.at[k, 0], ups),
            remote(got.at[k, span(across * chunk + part, part)], b1.at[k, 1], b_s.at[k, 1], b_r.at[k, 1], downs),
            remote(got.at[k, span(up * chunk + part, part)], b2.at[k, 0, pl.ds(part, part)], b_s.at[k, 2], b_r.at[k, 2], ups),
            remote(got.at[k, span(down * chunk, part)], b2.at[k, 1, pl.ds(0, part)], b_s.at[k, 3], b_r.at[k, 3], downs),
            remote(got.at[k, span(up * chunk, part)], b2.at[k, 0, pl.ds(0, part)], b_s.at[k, 4], b_r.at[k, 4], ups),
            remote(got.at[k, span(down * chunk + part, part)], b2.at[k, 1, pl.ds(part, part)], b_s.at[k, 5], b_r.at[k, 5], downs),
        )

    def copies_c(k):
        return [remote(ub.at[k, e], cr.at[k, e], c_s.at[k, e], c_r.at[k, e], others[e]) for e in range(side - 1)]

    def piece(k, start, size):
        return out.at[k, span(start, size), mine]

    def copies_d(k):
        dst = piece(k, p1 * chunk + p2 * sub, sub)
        return [remote(fb.at[k], dst, d_s.at[k, e], d_r.at[k, e], others[e]) for e in range(side - 1)]

    def copy_o(k):
        return pltpu.make_async_copy(fb.at[k], piece(k, p1 * chunk + p2 * sub, sub), o_sem.at[k])

    def shift(k, start, size, i, to):
        return remote(piece(k, start, size), piece(k, start, size), e_s.at[k, i], e_r.at[k, i], to)

    def copies_e(k):
        return (
            shift(k, p1 * chunk, part, 0, ups),
            shift(k, p1 * chunk + part, part, 1, downs),
            shift(k, p1 * chunk + part, part, 2, ups),
            shift(k, p1 * chunk, part, 3, downs),
            shift(k, down * chunk, part, 4, ups),
            shift(k, up * chunk + part, part, 5, downs),
        )

    def copies_f(k):
        return [
            remote(piece(k, q * chunk, chunk), piece(k, q * chunk, chunk), f_s.at[k, i], f_r.at[k, i], mate)
            for i, q in enumerate((p1, down, up, across))
        ]

    def load(k, which):
        slot = k % 2
        if which == "left":
            return lambda i: pltpu.make_async_copy(left_refs[lefts[i]], lv.at[slot], l_sem.at[slot])
        return lambda i: pltpu.make_async_copy(right_refs[rights[i]].at[:, theirs if which == 0 else mine], rv.at[which], r_sem.at[which])

    def start_load(k, which):
        for i in range(count):

            @pl.when(k == i)
            def _():
                load(k, which)(i).start()

    def dot(k, which, dst):
        block = 256 if rows % 256 == 0 else rows

        def body(j, _):
            r = pl.ds(pl.multiple_of(j * block, block), block)
            dst[r, :] = jnp.dot(lv[k % 2, r, :], rv[which], preferred_element_type=F32).astype(BF16)
            return 0

        lax.fori_loop(0, rows // block, body, 0)

    def add(start, size, dst, *terms):
        def body(j, _):
            total = None
            for ref, first in terms:
                one = ref[span(first + j * sub, sub), :].astype(F32)
                total = one if total is None else total + one
            dst[span(start + j * sub, sub), :] = total.astype(BF16)
            return 0

        lax.fori_loop(0, size // sub, body, 0)

    def step(s, k):
        g, r = own.at[k], got.at[k]
        if s == 0:

            @pl.when(k >= 2)
            def _():
                copy_a(k - 2).wait_send()

            load(k, "left")(0).wait()
            load(k, 0)(0).wait()
            dot(k, 0, other.at[k % 2])
            copy_a(k).start()

            @pl.when(k + 1 < count)
            def _():
                start_load(k + 1, "left")
                start_load(k + 1, 0)

            load(k, 1)(0).wait()
            dot(k, 1, g)

            @pl.when(k + 1 < count)
            def _():
                start_load(k + 1, 1)
        elif s == 1:
            copy_a(k).wait_recv()
            b = copies_b(k)
            add(across * chunk, chunk, r, (g, across * chunk), (r, across * chunk))
            b[0].start()
            b[1].start()
            add(up * chunk + part, part, r, (g, up * chunk + part), (r, up * chunk + part))
            b[2].start()
            add(down * chunk, part, r, (g, down * chunk), (r, down * chunk))
            b[3].start()
        elif s == 2:
            b = copies_b(k)
            b[0].wait_recv()
            add(up * chunk, part, r, (g, up * chunk), (r, up * chunk), (b1.at[k, 0], 0))
            b[4].start()
            b[1].wait_recv()
            add(down * chunk + part, part, r, (g, down * chunk + part), (r, down * chunk + part), (b1.at[k, 1], 0))
            b[5].start()
        elif s == 3:
            for one in copies_b(k)[2:]:
                one.wait_recv()
            for e, one in enumerate(copies_c(k)):
                at_sub = (p2 + e + 1) % side * sub
                first = p1 * chunk + at_sub
                add(0, sub, ub.at[k, e], (g, first), (r, first), (b2.at[k, 0], at_sub), (b2.at[k, 1], at_sub))
                one.start()
        elif s == 4:
            for one in copies_c(k):
                one.wait_recv()
            first = p1 * chunk + p2 * sub
            add(
                0, sub, fb.at[k], (g, first), (r, first), (b2.at[k, 0], p2 * sub), (b2.at[k, 1], p2 * sub),
                *[(cr.at[k, e], 0) for e in range(side - 1)],
            )
            for one in copies_d(k):
                one.start()
            copy_o(k).start()
        elif s == 5:
            copy_o(k).wait()
            for one in copies_d(k):
                one.wait_recv()
            for one in copies_e(k)[:4]:
                one.start()
            copies_f(k)[0].start()
        elif s == 6:
            e = copies_e(k)
            e[0].wait_recv()
            e[4].start()
            e[1].wait_recv()
            e[5].start()
        elif s == 7:
            for one in copies_e(k)[2:]:
                one.wait_recv()
            for one in copies_f(k)[1:]:
                one.start()
        elif s == 8:

            @pl.when(k + 2 >= count)
            def _():
                copy_a(k).wait_send()

            for one in copies_f(k):
                one.wait()
            for one in (*copies_b(k), *copies_c(k), *copies_d(k), *copies_e(k)):
                one.wait_send()

    for which in ("left", 0, 1):
        load(0, which)(0).start()

    def stage(t, _):
        for s in reversed(range(STEPS)):

            @pl.when(jnp.logical_and(t >= s, t - s < count))
            def _():
                step(s, t - s)

        return 0

    lax.fori_loop(0, count + STEPS - 1, stage, 0)


def summed(side, lefts, rights, layout):
    count = len(rights)
    (rows, tokens), columns = lefts[0].shape, rights[0].shape[1]
    half, chunk, sub = columns // 2, rows // side, rows // side // side
    vmem = lambda *shape: pltpu.VMEM(shape, BF16)
    sems = lambda *shape: pltpu.SemaphoreType.DMA(shape)
    hbm = pl.BlockSpec(memory_space=pltpu.HBM)
    return pl.pallas_call(
        functools.partial(summed_kernel, side, count, layout),
        out_shape=jax.ShapeDtypeStruct((count, rows, columns), BF16),
        in_specs=[hbm] * (len(lefts) + count),
        out_specs=hbm,
        scratch_shapes=[
            vmem(2, rows, tokens), vmem(2, tokens, half), vmem(2, rows, half), vmem(count, rows, half), vmem(count, rows, half),
            vmem(count, 2, chunk // 2, half), vmem(count, 2, chunk, half), vmem(count, side - 1, sub, half),
            vmem(count, side - 1, sub, half), vmem(count, sub, half),
            sems(2), sems(2), sems(count), sems(count), sems(count, 6), sems(count, 6), sems(count, side - 1), sems(count, side - 1),
            sems(count, side - 1), sems(count, side - 1), sems(count, 6), sems(count, 6), sems(count, 4), sems(count, 4), sems(count),
        ],
        compiler_params=pltpu.CompilerParams(collective_id=0, has_side_effects=True, vmem_limit_bytes=60 * 2**20),
        cost_estimate=pl.CostEstimate(flops=2 * count * rows * tokens * columns, bytes_accessed=0, transcendentals=0),
        name="summed_gradients",
    )(*lefts, *rights)


def adamw(w, m, v, g):
    m = 0.9 * m + 0.1 * g
    v = 0.95 * v + 0.05 * g * g
    step = m * lax.rsqrt(v + 1e-8) + 0.1 * w
    return (w - 0.02 * step).astype(BF16), m, v


def adamw_kernel(turned, g_ref, w_ref, m_ref, v_ref, ow, om, ov):
    g = g_ref[...].astype(F32)
    ow[...], om[...], ov[...] = adamw(w_ref[...].astype(F32), m_ref[...], v_ref[...], g.T if turned else g)


def adamw_all(places, turned, g, w, m, v):
    layers, rows, columns = w.shape
    block = 96 if not turned else 256
    if layers == 2:
        where = lambda l: places[0] + l * (places[1] - places[0])
    else:
        where = lambda l: sum(jnp.where(l == i, p, 0) for i, p in enumerate(places))
    of = pl.BlockSpec((None, block, columns), lambda l, i: (l, i, 0))
    if turned:
        g_of = pl.BlockSpec((None, columns, block), lambda l, i: (where(l), 0, i))
    else:
        g_of = pl.BlockSpec((None, block, columns), lambda l, i: (where(l), i, 0))
    return pl.pallas_call(
        functools.partial(adamw_kernel, turned),
        grid=(layers, rows // block),
        in_specs=[g_of, of, of, of],
        out_specs=[of] * 3,
        out_shape=[jax.ShapeDtypeStruct(a.shape, a.dtype) for a in (w, m, v)],
        cost_estimate=pl.CostEstimate(flops=layers * rows * columns * 15, bytes_accessed=layers * rows * columns * 22, transcendentals=0),
        name="adamw",
    )(g, w, m, v)


def matmul(a, w, turn=False):
    return lax.dot_general(a, w, (((1,), (1 if turn else 0,)), ((), ())), preferred_element_type=F32)


def normed(h):
    wide = h.astype(F32)
    scale = lax.rsqrt(jnp.mean(wide**2, -1, keepdims=True) + 1e-6)
    return (wide * scale).astype(BF16), wide, scale


def solution(mesh):
    side = int(round((mesh.shape["dp"] // 2) ** 0.5))
    assert side == 4 and 2 * side * side == mesh.shape["dp"]

    def step(x, dy, *arrays):
        (w_gate, w_up, w_down), m, v = (arrays[i : i + 3] for i in (0, 3, 6))
        layers = w_gate.shape[0]
        h, saved = x[0], []
        for l in range(layers):
            a, wide, scale = normed(h)
            gate, up = matmul(a, w_gate[l]), matmul(a, w_up[l])
            sig = jax.nn.sigmoid(gate)
            hidden = (gate * sig * up).astype(BF16)
            saved.append((a, wide, scale, gate, up, sig, hidden))
            if l + 1 < layers:
                h = h + matmul(hidden, w_down[l]).astype(BF16)
        by_h, lefts, rights = dy[0], [], []
        for l in reversed(range(layers)):
            a, wide, scale, gate, up, sig, hidden = saved[l]
            by_hidden = matmul(by_h, w_down[l], True).astype(BF16).astype(F32)
            by_up = (by_hidden * gate * sig).astype(BF16)
            by_gate = (by_hidden * up * (sig + gate * sig * (1 - sig))).astype(BF16)
            lefts += [by_h.T, a.T]
            rights += [hidden, by_gate, by_up]
            if l:
                by_a = matmul(by_gate, w_gate[l], True).astype(BF16) + matmul(by_up, w_up[l], True).astype(BF16)
                by_a = by_a.astype(F32)
                by_wide = scale * by_a - scale**3 * wide * jnp.mean(by_a * wide, -1, keepdims=True)
                by_h = by_h + by_wide.astype(BF16)
        layout = [2 * (i // 3) + (i % 3 > 0) for i in range(3 * layers)], list(range(3 * layers))
        g = summed(side, lefts, rights, layout)
        new = [
            adamw_all([3 * (layers - 1 - l) + i for l in range(layers)], i == 0, g, w, m_, v_)
            for i, w, m_, v_ in ((1, w_gate, m[0], v[0]), (2, w_up, m[1], v[1]), (0, w_down, m[2], v[2]))
        ]
        return tuple(one[which] for which in range(3) for one in new)

    return jax.shard_map(
        step,
        mesh=mesh,
        in_specs=(P(("rep", "dp"), None, None),) * 2 + (P(None, None, None),) * 9,
        out_specs=(P("rep", None, None),) * 9,
        check_vma=False,
    )
```

```python
import functools

import jax
import jax.numpy as jnp
from jax import lax
from jax.experimental import pallas as pl
from jax.experimental.pallas import tpu as pltpu
from jax.sharding import PartitionSpec as P

F32, BF16 = jnp.float32, jnp.bfloat16
STEPS = 9


class Copy:
    def __init__(self, describe):
        self.describe = describe

    def __getattr__(self, name):
        return getattr(self.describe(), name)


def summed_kernel(side, count, layout, *refs):
    lefts, rights = layout
    n_in = max(lefts) + 1 + count
    left_refs, right_refs, out = refs[: max(lefts) + 1], refs[max(lefts) + 1 : n_in], refs[n_in]
    (lv, rv, other, own, got, b1, b2, ub, cr, fb, l_sem, r_sem, a_s, a_r, b_s, b_r, c_s, c_r, d_s, d_r, e_s, e_r, f_s, f_r, o_sem) = refs[n_in + 1 :]
    rows, half = own.shape[1:]
    chunk, sub = rows // side, rows // side // side
    lo, hi = sub, chunk - sub

    me = lax.axis_index("dp")
    core = me % 2
    x, y = me // (2 * side), me // 2 % side
    p1, p2 = x * (1 - core) + y * core, y * (1 - core) + x * core
    far, near = 2 * side * (1 - core) + 2 * core, 2 * (1 - core) + 2 * side * core

    def at(q1, q2):
        return {"dp": q1 * far + q2 * near + core}

    up, down, across = (p1 + 1) % side, (p1 + side - 1) % side, (p1 + 2) % side
    mate = {"dp": me + 1 - 2 * core}
    ups, downs = at(up, p2), at(down, p2)
    others = [at(p1, (p2 + e) % side) for e in range(1, side)]

    barrier = pltpu.get_barrier_semaphore()
    peers = [mate, ups, downs] + others
    for peer in peers:
        pl.semaphore_signal(barrier, inc=1, device_id=peer, device_id_type=pl.DeviceIdType.MESH)
    pl.semaphore_wait(barrier, len(peers))

    mine = pl.ds(pl.multiple_of(core * half, 128), half)
    theirs = pl.ds(pl.multiple_of((1 - core) * half, 128), half)

    def span(start, size):
        return pl.ds(pl.multiple_of(start, 16), size)

    def remote(src, dst, send, recv, to):
        return Copy(
            lambda: pltpu.make_async_remote_copy(
                src_ref=src, dst_ref=dst, send_sem=send, recv_sem=recv, device_id=to, device_id_type=pl.DeviceIdType.MESH
            )
        )

    def copy_a(k):
        return remote(other.at[k % 2], got.at[k], a_s.at[k], a_r.at[k], mate)

    def copies_b(k):
        return (
            remote(got.at[k, span(across * chunk, lo)], b1.at[k, pl.ds(0, lo)], b_s.at[k, 0], b_r.at[k, 0], ups),
            remote(got.at[k, span(across * chunk + lo, hi)], b1.at[k, pl.ds(lo, hi)], b_s.at[k, 1], b_r.at[k, 1], downs),
            remote(got.at[k, span(up * chunk + lo, hi)], b2.at[k, 0, pl.ds(lo, hi)], b_s.at[k, 2], b_r.at[k, 2], ups),
            remote(got.at[k, span(down * chunk, lo)], b2.at[k, 1, pl.ds(0, lo)], b_s.at[k, 3], b_r.at[k, 3], downs),
            remote(got.at[k, span(up * chunk, lo)], b2.at[k, 0, pl.ds(0, lo)], b_s.at[k, 4], b_r.at[k, 4], ups),
            remote(got.at[k, span(down * chunk + lo, hi)], b2.at[k, 1, pl.ds(lo, hi)], b_s.at[k, 5], b_r.at[k, 5], downs),
        )

    def copies_c(k):
        return [remote(ub.at[k, e], cr.at[k, e], c_s.at[k, e], c_r.at[k, e], others[e]) for e in range(side - 1)]

    def piece(k, start, size):
        return out.at[k, span(start, size), mine]

    def copies_d(k):
        dst = piece(k, p1 * chunk + p2 * sub, sub)
        return [remote(fb.at[k], dst, d_s.at[k, e], d_r.at[k, e], others[e]) for e in range(side - 1)]

    def copy_o(k):
        return pltpu.make_async_copy(fb.at[k], piece(k, p1 * chunk + p2 * sub, sub), o_sem.at[k])

    def shift(k, start, size, i, to):
        return remote(piece(k, start, size), piece(k, start, size), e_s.at[k, i], e_r.at[k, i], to)

    def copies_e(k):
        return (
            shift(k, p1 * chunk, lo, 0, ups),
            shift(k, p1 * chunk + lo, hi, 1, downs),
            shift(k, p1 * chunk + lo, hi, 2, ups),
            shift(k, p1 * chunk, lo, 3, downs),
            shift(k, down * chunk, lo, 4, ups),
            shift(k, up * chunk + lo, hi, 5, downs),
        )

    def copies_f(k):
        return [
            remote(piece(k, q * chunk, chunk), piece(k, q * chunk, chunk), f_s.at[k, i], f_r.at[k, i], mate)
            for i, q in enumerate((p1, down, up, across))
        ]

    def load(k, which):
        slot = k % 2
        if which == "left":
            return lambda i: pltpu.make_async_copy(left_refs[lefts[i]], lv.at[slot], l_sem.at[slot])
        return lambda i: pltpu.make_async_copy(right_refs[rights[i]].at[:, theirs if which == 0 else mine], rv.at[which], r_sem.at[which])

    def start_load(k, which):
        for i in range(count):

            @pl.when(k == i)
            def _():
                load(k, which)(i).start()

    def dot(k, which, dst):
        block = 256 if rows % 256 == 0 else rows

        def body(j, _):
            r = pl.ds(pl.multiple_of(j * block, block), block)
            dst[r, :] = jnp.dot(lv[k % 2, r, :], rv[which], preferred_element_type=F32).astype(BF16)
            return 0

        lax.fori_loop(0, rows // block, body, 0)

    def add(start, size, dst, *terms):
        def body(j, _):
            total = None
            for ref, first in terms:
                one = ref[span(first + j * sub, sub), :].astype(F32)
                total = one if total is None else total + one
            dst[span(start + j * sub, sub), :] = total.astype(BF16)
            return 0

        lax.fori_loop(0, size // sub, body, 0)

    def step(s, k):
        g, r = own.at[k], got.at[k]
        if s == 0:

            @pl.when(k >= 2)
            def _():
                copy_a(k - 2).wait_send()

            load(k, "left")(0).wait()
            load(k, 0)(0).wait()
            dot(k, 0, other.at[k % 2])
            copy_a(k).start()

            @pl.when(k + 1 < count)
            def _():
                start_load(k + 1, "left")
                start_load(k + 1, 0)

            load(k, 1)(0).wait()
            dot(k, 1, g)

            @pl.when(k + 1 < count)
            def _():
                start_load(k + 1, 1)
        elif s == 1:
            copy_a(k).wait_recv()
            b = copies_b(k)
            add(across * chunk, chunk, r, (g, across * chunk), (r, across * chunk))
            b[0].start()
            b[1].start()
            add(up * chunk + lo, hi, r, (g, up * chunk + lo), (r, up * chunk + lo))
            b[2].start()
            add(down * chunk, lo, r, (g, down * chunk), (r, down * chunk))
            b[3].start()
        elif s == 2:
            b = copies_b(k)
            b[0].wait_recv()
            add(up * chunk, lo, r, (g, up * chunk), (r, up * chunk), (b1.at[k], 0))
            b[4].start()
            b[1].wait_recv()
            add(down * chunk + lo, hi, r, (g, down * chunk + lo), (r, down * chunk + lo), (b1.at[k], lo))
            b[5].start()
        elif s == 3:
            for one in copies_b(k)[2:]:
                one.wait_recv()
            for e, one in enumerate(copies_c(k)):
                at_sub = (p2 + e + 1) % side * sub
                first = p1 * chunk + at_sub
                add(0, sub, ub.at[k, e], (g, first), (r, first), (b2.at[k, 0], at_sub), (b2.at[k, 1], at_sub))
                one.start()
        elif s == 4:
            for one in copies_c(k):
                one.wait_recv()
            first = p1 * chunk + p2 * sub
            add(
                0, sub, fb.at[k], (g, first), (r, first), (b2.at[k, 0], p2 * sub), (b2.at[k, 1], p2 * sub),
                *[(cr.at[k, e], 0) for e in range(side - 1)],
            )
            for one in copies_d(k):
                one.start()
            copy_o(k).start()
        elif s == 5:
            copy_o(k).wait()
            for one in copies_d(k):
                one.wait_recv()
            for one in copies_e(k)[:4]:
                one.start()
            copies_f(k)[0].start()
        elif s == 6:
            e = copies_e(k)
            e[0].wait_recv()
            e[4].start()
            e[1].wait_recv()
            e[5].start()
        elif s == 7:
            for one in copies_e(k)[2:]:
                one.wait_recv()
            for one in copies_f(k)[1:]:
                one.start()
        elif s == 8:

            @pl.when(k + 2 >= count)
            def _():
                copy_a(k).wait_send()

            for one in copies_f(k):
                one.wait()
            for one in (*copies_b(k), *copies_c(k), *copies_d(k), *copies_e(k)):
                one.wait_send()

    for which in ("left", 0, 1):
        load(0, which)(0).start()

    def stage(t, _):
        for s in reversed(range(STEPS)):

            @pl.when(jnp.logical_and(t >= s, t - s < count))
            def _():
                step(s, t - s)

        return 0

    lax.fori_loop(0, count + STEPS - 1, stage, 0)


def summed(side, lefts, rights, layout):
    count = len(rights)
    (rows, tokens), columns = lefts[0].shape, rights[0].shape[1]
    half, chunk, sub = columns // 2, rows // side, rows // side // side
    vmem = lambda *shape: pltpu.VMEM(shape, BF16)
    sems = lambda *shape: pltpu.SemaphoreType.DMA(shape)
    hbm = pl.BlockSpec(memory_space=pltpu.HBM)
    return pl.pallas_call(
        functools.partial(summed_kernel, side, count, layout),
        out_shape=jax.ShapeDtypeStruct((count, rows, columns), BF16),
        in_specs=[hbm] * (len(lefts) + count),
        out_specs=hbm,
        scratch_shapes=[
            vmem(2, rows, tokens), vmem(2, tokens, half), vmem(2, rows, half), vmem(count, rows, half), vmem(count, rows, half),
            vmem(count, chunk, half), vmem(count, 2, chunk, half), vmem(count, side - 1, sub, half),
            vmem(count, side - 1, sub, half), vmem(count, sub, half),
            sems(2), sems(2), sems(count), sems(count), sems(count, 6), sems(count, 6), sems(count, side - 1), sems(count, side - 1),
            sems(count, side - 1), sems(count, side - 1), sems(count, 6), sems(count, 6), sems(count, 4), sems(count, 4), sems(count),
        ],
        compiler_params=pltpu.CompilerParams(collective_id=0, has_side_effects=True, vmem_limit_bytes=60 * 2**20),
        cost_estimate=pl.CostEstimate(flops=2 * count * rows * tokens * columns, bytes_accessed=0, transcendentals=0),
        name="summed_gradients",
    )(*lefts, *rights)


def adamw(w, m, v, g):
    m = 0.9 * m + 0.1 * g
    v = 0.95 * v + 0.05 * g * g
    step = m * lax.rsqrt(v + 1e-8) + 0.1 * w
    return (w - 0.02 * step).astype(BF16), m, v


def adamw_kernel(turned, *refs):
    n = len(turned)
    for i in range(n):
        (g, w, m, v), outs = refs[4 * i : 4 * i + 4], refs[4 * n + 3 * i : 4 * n + 3 * i + 3]
        g = g[...].astype(F32)
        results = adamw(w[...].astype(F32), m[...], v[...], g.T if turned[i] else g)
        for out, result in zip(outs, results, strict=True):
            out[...] = result


def adamw_all(g, starts, turned, weights, m, v, parts):
    layers = weights[0].shape[0]
    in_specs, out_specs, shapes, operands, bytes_moved = [], [], [], [], 0
    for i, (w, first) in enumerate(zip(weights, starts, strict=True)):
        _, rows, columns = w.shape
        block = rows // parts
        of = pl.BlockSpec((None, block, columns), lambda l, j: (l, j, 0))
        if turned[i]:
            g_of = pl.BlockSpec((None, columns, block), lambda l, j, first=first: (first[0] + first[1] * l, 0, j))
        else:
            g_of = pl.BlockSpec((None, block, columns), lambda l, j, first=first: (first[0] + first[1] * l, j, 0))
        in_specs += [g_of, of, of, of]
        out_specs += [of] * 3
        shapes += [jax.ShapeDtypeStruct(a.shape, a.dtype) for a in (w, m[i], v[i])]
        operands += [g, w, m[i], v[i]]
        bytes_moved += 22 * layers * rows * columns
    new = pl.pallas_call(
        functools.partial(adamw_kernel, turned),
        grid=(layers, parts),
        in_specs=in_specs,
        out_specs=out_specs,
        out_shape=shapes,
        compiler_params=pltpu.CompilerParams(vmem_limit_bytes=60 * 2**20),
        cost_estimate=pl.CostEstimate(flops=bytes_moved, bytes_accessed=bytes_moved, transcendentals=0),
        name="adamw",
    )(*operands)
    return [new[3 * i : 3 * i + 3] for i in range(len(weights))]


def dot(a, w, turn=False):
    return lax.dot_general(a, w, (((1,), (1 if turn else 0,)), ((), ())), preferred_element_type=F32)


def rounded(value):
    return value.astype(BF16).astype(F32)


def normed(h):
    wide = h.astype(F32)
    scale = lax.rsqrt(jnp.mean(wide**2, -1, keepdims=True) + 1e-6)
    return (wide * scale).astype(BF16), wide, scale


def local_kernel(x_ref, dy_ref, gate_hbm, up_hbm, down_hbm, *refs):
    turned, (hidden0, gate0, up0, hidden1, gate1, up1) = refs[:4], refs[4:10]
    wg, wu, wd, s0, p0, sem = refs[10:]
    columns = wg.shape[2]
    block = columns // 3
    blocks = [pl.ds(j * block, block) for j in range(3)]
    first = pl.program_id(0) == 0

    def copy(i):
        source, target = ((gate_hbm, wg), (up_hbm, wu), (down_hbm, wd))[i % 3]
        return pltpu.make_async_copy(source.at[i // 3], target.at[i // 3], sem.at[i])

    @pl.when(first)
    def _():
        for i in range(6):
            copy(i).start()

    def have(*which):
        @pl.when(first)
        def _():
            for i in which:
                copy(i).wait()

    dy_turned, a1_turned, dh1_turned, a0_turned = turned
    x, dy = x_ref[...], dy_ref[...]
    a0, _, _ = normed(x)
    a0_turned[...] = a0.T
    dy_turned[...] = dy.T
    have(0, 1)
    for c in blocks:
        gate, up = dot(a0, wg[0, :, c]), dot(a0, wu[0, :, c])
        sig = jax.nn.sigmoid(gate)
        silu = gate * sig
        hidden0[:, c] = (silu * up).astype(BF16)
        s0[:, c] = silu
        p0[:, c] = up * (sig + silu * (1 - sig))
    have(2)
    h = (x.astype(F32) + rounded(dot(hidden0[...], wd[0]))).astype(BF16)
    a1, wide, scale = normed(h)
    a1_turned[...] = a1.T
    have(3, 4, 5)
    for j, c in enumerate(blocks):
        gate, up = dot(a1, wg[1, :, c]), dot(a1, wu[1, :, c])
        by_hidden = rounded(dot(dy, wd[1, c, :], True))
        sig = jax.nn.sigmoid(gate)
        silu = gate * sig
        hidden1[:, c] = (silu * up).astype(BF16)
        up1[:, c] = (by_hidden * silu).astype(BF16)
        gate1[:, c] = (by_hidden * up * (sig + silu * (1 - sig))).astype(BF16)
    by_a = rounded(rounded(dot(gate1[...], wg[1], True)) + rounded(dot(up1[...], wu[1], True)))
    by_wide = scale * by_a - scale**3 * wide * jnp.mean(by_a * wide, -1, keepdims=True)
    by_h = (dy.astype(F32) + rounded(by_wide)).astype(BF16)
    dh1_turned[...] = by_h.T
    for c in blocks:
        by_hidden = rounded(dot(by_h, wd[0, c, :], True))
        up0[:, c] = (by_hidden * s0[:, c]).astype(BF16)
        gate0[:, c] = (by_hidden * p0[:, c]).astype(BF16)


def local(x, dy, w_gate, w_up, w_down):
    (tokens, d), (layers, _, columns) = x.shape, w_gate.shape
    assert layers == 2
    block = min(256, tokens)
    of = lambda width: pl.BlockSpec((block, width), lambda i: (i, 0))
    turned = pl.BlockSpec((d, block), lambda i: (0, i))
    hbm = pl.BlockSpec(memory_space=pltpu.HBM)
    shape = lambda *s: jax.ShapeDtypeStruct(s, BF16)
    return pl.pallas_call(
        local_kernel,
        grid=(tokens // block,),
        in_specs=[of(d), of(d), hbm, hbm, hbm],
        out_specs=[turned] * 4 + [of(columns)] * 6,
        out_shape=[shape(d, tokens)] * 4 + [shape(tokens, columns)] * 6,
        scratch_shapes=[pltpu.VMEM(w.shape, BF16) for w in (w_gate, w_up, w_down)]
        + [pltpu.VMEM((block, columns), F32)] * 2
        + [pltpu.SemaphoreType.DMA((6,))],
        compiler_params=pltpu.CompilerParams(vmem_limit_bytes=60 * 2**20),
        cost_estimate=pl.CostEstimate(flops=18 * tokens * d * columns, bytes_accessed=0, transcendentals=0),
        name="local_parts",
    )(x, dy, w_gate, w_up, w_down)


def solution(mesh):
    side = int(round((mesh.shape["dp"] // 2) ** 0.5))
    assert side == 4 and 2 * side * side == mesh.shape["dp"]

    def step(x, dy, *arrays):
        weights, m, v = (arrays[i : i + 3] for i in (0, 3, 6))
        layers = weights[0].shape[0]
        dy_turned, a1_turned, dh1_turned, a0_turned, hidden0, gate0, up0, hidden1, gate1, up1 = local(x[0], dy[0], *weights)
        lefts = [dy_turned, a1_turned, dh1_turned, a0_turned]
        g = summed(side, lefts, [hidden1, gate1, up1, hidden0, gate0, up0], ([0, 1, 1, 2, 3, 3], list(range(6))))
        last = 3 * (layers - 1)
        new = adamw_all(g, [(last + i, -3) for i in (1, 2, 0)], (False, False, True), weights, m, v, 6)
        return tuple(one[which] for which in range(3) for one in new)

    return jax.shard_map(
        step,
        mesh=mesh,
        in_specs=(P(("rep", "dp"), None, None),) * 2 + (P(None, None, None),) * 9,
        out_specs=(P("rep", None, None),) * 9,
        check_vma=False,
    )
```

```python
import functools

import jax
import jax.numpy as jnp
from jax import lax
from jax.experimental import pallas as pl
from jax.experimental.pallas import tpu as pltpu
from jax.sharding import PartitionSpec as P

F32, BF16 = jnp.float32, jnp.bfloat16
STEPS = 9
SPLIT = 1


class Copy:
    def __init__(self, describe):
        self.describe = describe

    def __getattr__(self, name):
        return getattr(self.describe(), name)


def summed_kernel(side, gradients, layout, *refs):
    lefts, rights = layout
    n_in = max(lefts) + 1 + gradients
    count = gradients * SPLIT
    left_refs, right_refs, out = refs[: max(lefts) + 1], refs[max(lefts) + 1 : n_in], refs[n_in]
    (lv, rv, other, own, got, b1, b2, ub, cr, fb, l_sem, r_sem, a_s, a_r, b_s, b_r, c_s, c_r, d_s, d_r, e_s, e_r, f_s, f_r, o_sem) = refs[n_in + 1 :]
    rows, half = own.shape[1:]
    chunk, sub = rows // side, rows // side // side
    lo = hi = chunk // 2

    me = lax.axis_index("dp")
    core = me % 2
    x, y = me // (2 * side), me // 2 % side
    p1, p2 = x * (1 - core) + y * core, y * (1 - core) + x * core
    far, near = 2 * side * (1 - core) + 2 * core, 2 * (1 - core) + 2 * side * core

    def at(q1, q2):
        return {"dp": q1 * far + q2 * near + core}

    up, down, across = (p1 + 1) % side, (p1 + side - 1) % side, (p1 + 2) % side
    mate = {"dp": me + 1 - 2 * core}
    ups, downs = at(up, p2), at(down, p2)
    others = [at(p1, (p2 + e) % side) for e in range(1, side)]

    def columns(k, which):
        place = k % SPLIT * 2 * half + (core if which else 1 - core) * half
        return pl.ds(pl.multiple_of(place, 128), half)

    def span(start, size):
        return pl.ds(pl.multiple_of(start, 16), size)

    def remote(src, dst, send, recv, to):
        return Copy(
            lambda: pltpu.make_async_remote_copy(
                src_ref=src, dst_ref=dst, send_sem=send, recv_sem=recv, device_id=to, device_id_type=pl.DeviceIdType.MESH
            )
        )

    def copy_a(k):
        return remote(other.at[k % 2], got.at[k], a_s.at[k], a_r.at[k], mate)

    def copies_b(k):
        return (
            remote(got.at[k, span(across * chunk, lo)], b1.at[k, pl.ds(0, lo)], b_s.at[k, 0], b_r.at[k, 0], ups),
            remote(got.at[k, span(across * chunk + lo, hi)], b1.at[k, pl.ds(lo, hi)], b_s.at[k, 1], b_r.at[k, 1], downs),
            remote(got.at[k, span(up * chunk + lo, hi)], b2.at[k, 0, pl.ds(lo, hi)], b_s.at[k, 2], b_r.at[k, 2], ups),
            remote(got.at[k, span(down * chunk, lo)], b2.at[k, 1, pl.ds(0, lo)], b_s.at[k, 3], b_r.at[k, 3], downs),
            remote(got.at[k, span(up * chunk, lo)], b2.at[k, 0, pl.ds(0, lo)], b_s.at[k, 4], b_r.at[k, 4], ups),
            remote(got.at[k, span(down * chunk + lo, hi)], b2.at[k, 1, pl.ds(lo, hi)], b_s.at[k, 5], b_r.at[k, 5], downs),
        )

    def copies_c(k):
        return [remote(ub.at[k, e], cr.at[k, e], c_s.at[k, e], c_r.at[k, e], others[e]) for e in range(side - 1)]

    def piece(k, start, size):
        return out.at[k // SPLIT, span(start, size), columns(k, 1)]

    def copies_d(k):
        dst = piece(k, p1 * chunk + p2 * sub, sub)
        return [remote(fb.at[k], dst, d_s.at[k, e], d_r.at[k, e], others[e]) for e in range(side - 1)]

    def copy_o(k):
        return pltpu.make_async_copy(fb.at[k], piece(k, p1 * chunk + p2 * sub, sub), o_sem.at[k])

    def shift(k, start, size, i, to):
        return remote(piece(k, start, size), piece(k, start, size), e_s.at[k, i], e_r.at[k, i], to)

    def copies_e(k):
        return (
            shift(k, p1 * chunk, lo, 0, ups),
            shift(k, p1 * chunk + lo, hi, 1, downs),
            shift(k, p1 * chunk + lo, hi, 2, ups),
            shift(k, p1 * chunk, lo, 3, downs),
            shift(k, down * chunk, lo, 4, ups),
            shift(k, up * chunk + lo, hi, 5, downs),
        )

    def copies_f(k):
        return [
            remote(piece(k, q * chunk, chunk), piece(k, q * chunk, chunk), f_s.at[k, i], f_r.at[k, i], mate)
            for i, q in enumerate((p1, down, up, across))
        ]

    def load(k, which, i=0):
        if which == "left":
            slot = k // SPLIT % 2
            return pltpu.make_async_copy(left_refs[lefts[i]], lv.at[slot], l_sem.at[slot])
        return pltpu.make_async_copy(right_refs[rights[i]].at[:, columns(k, which)], rv.at[which], r_sem.at[which])

    def start_load(k, which):
        for i in range(gradients):

            @pl.when(k // SPLIT == i)
            def _():
                load(k, which, i).start()

    def dot(k, which, dst):
        block = 256 if rows % 256 == 0 else rows

        def body(j, _):
            r = pl.ds(pl.multiple_of(j * block, block), block)
            dst[r, :] = jnp.dot(lv[k // SPLIT % 2, r, :], rv[which], preferred_element_type=F32).astype(BF16)
            return 0

        lax.fori_loop(0, rows // block, body, 0)

    def add(start, size, dst, *terms):
        def body(j, _):
            total = None
            for ref, first in terms:
                one = ref[span(first + j * sub, sub), :].astype(F32)
                total = one if total is None else total + one
            dst[span(start + j * sub, sub), :] = total.astype(BF16)
            return 0

        lax.fori_loop(0, size // sub, body, 0)

    def step(s, k):
        g, r = own.at[k], got.at[k]
        if s == 0:

            @pl.when(k >= 2)
            def _():
                copy_a(k - 2).wait_send()

            @pl.when(k % SPLIT == 0)
            def _():
                load(k, "left").wait()

            load(k, 0).wait()
            dot(k, 0, other.at[k % 2])
            copy_a(k).start()

            @pl.when(jnp.logical_and((k + 1) % SPLIT == 0, k + 1 < count))
            def _():
                start_load(k + 1, "left")

            @pl.when(k + 1 < count)
            def _():
                start_load(k + 1, 0)

            load(k, 1).wait()
            dot(k, 1, g)

            @pl.when(k + 1 < count)
            def _():
                start_load(k + 1, 1)
        elif s == 1:
            copy_a(k).wait_recv()
            b = copies_b(k)
            add(across * chunk, chunk, r, (g, across * chunk), (r, across * chunk))
            b[0].start()
            b[1].start()
            add(up * chunk + lo, hi, r, (g, up * chunk + lo), (r, up * chunk + lo))
            b[2].start()
            add(down * chunk, lo, r, (g, down * chunk), (r, down * chunk))
            b[3].start()
        elif s == 2:
            b = copies_b(k)
            b[0].wait_recv()
            add(up * chunk, lo, r, (g, up * chunk), (r, up * chunk), (b1.at[k], 0))
            b[4].start()
            b[1].wait_recv()
            add(down * chunk + lo, hi, r, (g, down * chunk + lo), (r, down * chunk + lo), (b1.at[k], lo))
            b[5].start()
        elif s == 3:
            for one in copies_b(k)[2:]:
                one.wait_recv()
            for e, one in enumerate(copies_c(k)):
                at_sub = (p2 + e + 1) % side * sub
                first = p1 * chunk + at_sub
                add(0, sub, ub.at[k, e], (g, first), (r, first), (b2.at[k, 0], at_sub), (b2.at[k, 1], at_sub))
                one.start()
        elif s == 4:
            for one in copies_c(k):
                one.wait_recv()
            first = p1 * chunk + p2 * sub
            add(
                0, sub, fb.at[k], (g, first), (r, first), (b2.at[k, 0], p2 * sub), (b2.at[k, 1], p2 * sub),
                *[(cr.at[k, e], 0) for e in range(side - 1)],
            )
            for one in copies_d(k):
                one.start()
            copy_o(k).start()
        elif s == 5:
            copy_o(k).wait()
            for one in copies_d(k):
                one.wait_recv()
            for one in copies_e(k)[:4]:
                one.start()
            copies_f(k)[0].start()
        elif s == 6:
            e = copies_e(k)
            e[0].wait_recv()
            e[4].start()
            e[1].wait_recv()
            e[5].start()
        elif s == 7:
            for one in copies_e(k)[2:]:
                one.wait_recv()
            for one in copies_f(k)[1:]:
                one.start()
        elif s == 8:

            @pl.when(k + 2 >= count)
            def _():
                copy_a(k).wait_send()

            for one in copies_f(k):
                one.wait()
            for one in (*copies_b(k), *copies_c(k), *copies_d(k), *copies_e(k)):
                one.wait_send()

    for which in ("left", 0, 1):
        load(0, which).start()

    barrier = pltpu.get_barrier_semaphore()
    peers = [mate, ups, downs] + others
    for peer in peers:
        pl.semaphore_signal(barrier, inc=1, device_id=peer, device_id_type=pl.DeviceIdType.MESH)
    pl.semaphore_wait(barrier, len(peers))

    def stage(t, _):
        for s in reversed(range(STEPS)):

            @pl.when(jnp.logical_and(t >= s, t - s < count))
            def _():
                step(s, t - s)

        return 0

    lax.fori_loop(0, count + STEPS - 1, stage, 0)


def summed(side, lefts, rights, layout):
    gradients = len(rights)
    count = gradients * SPLIT
    (rows, tokens), columns = lefts[0].shape, rights[0].shape[1]
    half, chunk, sub = columns // SPLIT // 2, rows // side, rows // side // side
    vmem = lambda *shape: pltpu.VMEM(shape, BF16)
    sems = lambda *shape: pltpu.SemaphoreType.DMA(shape)
    hbm = pl.BlockSpec(memory_space=pltpu.HBM)
    return pl.pallas_call(
        functools.partial(summed_kernel, side, gradients, layout),
        out_shape=jax.ShapeDtypeStruct((gradients, rows, columns), BF16),
        in_specs=[hbm] * (len(lefts) + gradients),
        out_specs=hbm,
        scratch_shapes=[
            vmem(2, rows, tokens), vmem(2, tokens, half), vmem(2, rows, half), vmem(count, rows, half), vmem(count, rows, half),
            vmem(count, chunk, half), vmem(count, 2, chunk, half), vmem(count, side - 1, sub, half),
            vmem(count, side - 1, sub, half), vmem(count, sub, half),
            sems(2), sems(2), sems(count), sems(count), sems(count, 6), sems(count, 6), sems(count, side - 1), sems(count, side - 1),
            sems(count, side - 1), sems(count, side - 1), sems(count, 6), sems(count, 6), sems(count, 4), sems(count, 4), sems(count),
        ],
        compiler_params=pltpu.CompilerParams(collective_id=0, has_side_effects=True, vmem_limit_bytes=60 * 2**20),
        cost_estimate=pl.CostEstimate(flops=2 * gradients * rows * tokens * columns, bytes_accessed=0, transcendentals=0),
        name="summed_gradients",
    )(*lefts, *rights)


def adamw(w, m, v, g):
    m = 0.9 * m + 0.1 * g
    v = 0.95 * v + 0.05 * g * g
    step = m * lax.rsqrt(v + 1e-8) + 0.1 * w
    return (w - 0.02 * step).astype(BF16), m, v


def adamw_kernel(turned, *refs):
    n = len(turned)
    for i in range(n):
        (g, w, m, v), outs = refs[4 * i : 4 * i + 4], refs[4 * n + 3 * i : 4 * n + 3 * i + 3]
        g = g[...].astype(F32)
        results = adamw(w[...].astype(F32), m[...], v[...], g.T if turned[i] else g)
        for out, result in zip(outs, results, strict=True):
            out[...] = result


def adamw_all(g, starts, turned, weights, m, v, parts):
    layers = weights[0].shape[0]
    in_specs, out_specs, shapes, operands, bytes_moved = [], [], [], [], 0
    for i, (w, first) in enumerate(zip(weights, starts, strict=True)):
        _, rows, columns = w.shape
        block = rows // parts
        of = pl.BlockSpec((None, block, columns), lambda l, j: (l, j, 0))
        if turned[i]:
            g_of = pl.BlockSpec((None, columns, block), lambda l, j, first=first: (first[0] + first[1] * l, 0, j))
        else:
            g_of = pl.BlockSpec((None, block, columns), lambda l, j, first=first: (first[0] + first[1] * l, j, 0))
        in_specs += [g_of, of, of, of]
        out_specs += [of] * 3
        shapes += [jax.ShapeDtypeStruct(a.shape, a.dtype) for a in (w, m[i], v[i])]
        operands += [g, w, m[i], v[i]]
        bytes_moved += 22 * layers * rows * columns
    new = pl.pallas_call(
        functools.partial(adamw_kernel, turned),
        grid=(layers, parts),
        in_specs=in_specs,
        out_specs=out_specs,
        out_shape=shapes,
        compiler_params=pltpu.CompilerParams(vmem_limit_bytes=60 * 2**20),
        cost_estimate=pl.CostEstimate(flops=bytes_moved, bytes_accessed=bytes_moved, transcendentals=0),
        name="adamw",
    )(*operands)
    return [new[3 * i : 3 * i + 3] for i in range(len(weights))]


TOKENS = 512


def dot(a, w, turn=False):
    return lax.dot_general(a, w, (((1,), (1 if turn else 0,)), ((), ())), preferred_element_type=F32)


def rounded(value):
    return value.astype(BF16).astype(F32)


def normed(h):
    wide = h.astype(F32)
    scale = lax.rsqrt(jnp.mean(wide**2, -1, keepdims=True) + 1e-6)
    return (wide * scale).astype(BF16), wide, scale


def local_kernel(x_ref, dy_ref, gate_hbm, up_hbm, down_hbm, *refs):
    turned, outs, buffers = refs[:4], refs[4:10], refs[10:16]
    hidden0, gate0, up0, hidden1, gate1, up1 = buffers
    wg, wu, wd, s0, p0, sem, out_sem = refs[16:]
    columns = wg.shape[2]
    block = columns // 3
    blocks = [pl.ds(j * block, block) for j in range(3)]
    now, steps = pl.program_id(0), pl.num_programs(0)
    first = now == 0
    rows = hidden0.shape[0]

    def put(i, step):
        at = pl.ds(pl.multiple_of(step * rows, 16), rows)
        return pltpu.make_async_copy(buffers[i], outs[i].at[at], out_sem.at[i])

    def free(*which):
        @pl.when(now > 0)
        def _():
            for i in which:
                put(i, now - 1).wait()

    def copy(i):
        source, target = ((gate_hbm, wg), (up_hbm, wu), (down_hbm, wd))[i % 3]
        return pltpu.make_async_copy(source.at[i // 3], target.at[i // 3], sem.at[i])

    @pl.when(first)
    def _():
        for i in range(6):
            copy(i).start()

    def have(*which):
        @pl.when(first)
        def _():
            for i in which:
                copy(i).wait()

    dy_turned, a1_turned, dh1_turned, a0_turned = turned
    x, dy = x_ref[...], dy_ref[...]
    a0, _, _ = normed(x)
    a0_turned[...] = a0.T
    dy_turned[...] = dy.T
    have(0, 1)
    free(0)
    for c in blocks:
        gate, up = dot(a0, wg[0, :, c]), dot(a0, wu[0, :, c])
        sig = jax.nn.sigmoid(gate)
        silu = gate * sig
        hidden0[:, c] = (silu * up).astype(BF16)
        s0[:, c] = silu
        p0[:, c] = up * (sig + silu * (1 - sig))
    put(0, now).start()
    have(2)
    h = (x.astype(F32) + rounded(dot(hidden0[...], wd[0]))).astype(BF16)
    a1, wide, scale = normed(h)
    a1_turned[...] = a1.T
    have(3, 4, 5)
    free(3, 4, 5)
    for j, c in enumerate(blocks):
        gate, up = dot(a1, wg[1, :, c]), dot(a1, wu[1, :, c])
        by_hidden = rounded(dot(dy, wd[1, c, :], True))
        sig = jax.nn.sigmoid(gate)
        silu = gate * sig
        hidden1[:, c] = (silu * up).astype(BF16)
        up1[:, c] = (by_hidden * silu).astype(BF16)
        gate1[:, c] = (by_hidden * up * (sig + silu * (1 - sig))).astype(BF16)
    for i in (3, 4, 5):
        put(i, now).start()
    by_a = rounded(rounded(dot(gate1[...], wg[1], True)) + rounded(dot(up1[...], wu[1], True)))
    by_wide = scale * by_a - scale**3 * wide * jnp.mean(by_a * wide, -1, keepdims=True)
    by_h = (dy.astype(F32) + rounded(by_wide)).astype(BF16)
    dh1_turned[...] = by_h.T
    free(1, 2)
    for c in blocks:
        by_hidden = rounded(dot(by_h, wd[0, c, :], True))
        up0[:, c] = (by_hidden * s0[:, c]).astype(BF16)
        gate0[:, c] = (by_hidden * p0[:, c]).astype(BF16)
    put(1, now).start()
    put(2, now).start()

    @pl.when(now == steps - 1)
    def _():
        for i in range(6):
            put(i, now).wait()


def local(x, dy, w_gate, w_up, w_down):
    (tokens, d), (layers, _, columns) = x.shape, w_gate.shape
    assert layers == 2
    block = min(TOKENS, tokens)
    of = lambda width: pl.BlockSpec((block, width), lambda i: (i, 0))
    turned = pl.BlockSpec((d, block), lambda i: (0, i))
    hbm = pl.BlockSpec(memory_space=pltpu.HBM)
    shape = lambda *s: jax.ShapeDtypeStruct(s, BF16)
    return pl.pallas_call(
        local_kernel,
        grid=(tokens // block,),
        in_specs=[of(d), of(d), hbm, hbm, hbm],
        out_specs=[turned] * 4 + [hbm] * 6,
        out_shape=[shape(d, tokens)] * 4 + [shape(tokens, columns)] * 6,
        scratch_shapes=[pltpu.VMEM((block, columns), BF16)] * 6
        + [pltpu.VMEM(w.shape, BF16) for w in (w_gate, w_up, w_down)]
        + [pltpu.VMEM((block, columns), F32)] * 2
        + [pltpu.SemaphoreType.DMA((6,))] * 2,
        compiler_params=pltpu.CompilerParams(vmem_limit_bytes=63 * 2**20),
        cost_estimate=pl.CostEstimate(flops=18 * tokens * d * columns, bytes_accessed=0, transcendentals=0),
        name="local_parts",
    )(x, dy, w_gate, w_up, w_down)


def solution(mesh):
    side = int(round((mesh.shape["dp"] // 2) ** 0.5))
    assert side == 4 and 2 * side * side == mesh.shape["dp"]

    def step(x, dy, *arrays):
        weights, m, v = (arrays[i : i + 3] for i in (0, 3, 6))
        layers = weights[0].shape[0]
        dy_turned, a1_turned, dh1_turned, a0_turned, hidden0, gate0, up0, hidden1, gate1, up1 = local(x[0], dy[0], *weights)
        lefts = [dy_turned, a1_turned, dh1_turned, a0_turned]
        g = summed(side, lefts, [hidden1, gate1, up1, hidden0, gate0, up0], ([0, 1, 1, 2, 3, 3], list(range(6))))
        last = 3 * (layers - 1)
        new = adamw_all(g, [(last + i, -3) for i in (1, 2, 0)], (False, False, True), weights, m, v, 6)
        return tuple(one[which] for which in range(3) for one in new)

    return jax.shard_map(
        step,
        mesh=mesh,
        in_specs=(P(("rep", "dp"), None, None),) * 2 + (P(None, None, None),) * 9,
        out_specs=(P("rep", None, None),) * 9,
        check_vma=False,
    )
```
